512 devices in a mesh: tok: 64 (over y, z), grp: 8 (over x, core).
Axes of the slice: x: 4, y: 8, z: 8, core: 2. Of those that a mesh axis runs over, the one named last changes fastest.
Arguments:
- acts: bfloat16 [8, 16384, 512], P('grp', 'tok'), may hold values from -16 to 16
- grads: bfloat16 [8, 16384, 512], P('grp', 'tok'), may hold values from -16 to 16
- tile_expert: int32 [8, 256], P('grp', 'tok'), may hold values from 0 to 1
- tile_rows: int32 [8, 256], P('grp', 'tok'), may hold values from 1 to 64
- previous: float32 [512, 16, 2, 512], P('tok', None, None, 'grp'), may hold values from -0.18 to 0.18
Outputs:
- statistics: float32 [512, 16, 2, 512], P('tok', None, None, 'grp')
The draws below stay inside these ranges and needn't reach their ends.
Inputs may be any that keep to these rules, and one draw needn't show every extreme that they name: `tile_expert`: the index of the tile's expert within its group. `tile_rows`: the live rows of a tile are its first rows.
All inputs are finite; a program needn't handle non-finite values.
Results may differ from the reference program's by a relative error of at most 0.0003.
Values sent between devices are 32-bit elements; how exact they have to be, the bound alone decides.
A program may use at most 64 MiB of HBM per device.

```python
import jax
import jax.numpy as jnp
from jax import lax

BLK = 512
EXP_GRP = 2
TROWS = 64
ROWS = 16384
TILES_ALL = 256
EXPERTS = 16
N_GRP = 8


def plant(values, rng, smallest, top_value):
    spot = [jax.random.randint(jax.random.fold_in(rng, axis), (), 0, length) for axis, length in enumerate(values.shape)]
    main_axis = values.shape.index(max(values.shape))
    neighbour = spot[:main_axis] + [(spot[main_axis] + 1) % values.shape[main_axis]] + spot[main_axis + 1:]
    return values.at[tuple(spot)].set(smallest).at[tuple(neighbour)].set(top_value)


def spiked(entries, own_key, source, target, parts, factor):
    owner, partner = [(jnp.arange(entries.shape[axis_at]) // (entries.shape[axis_at] // parts)).reshape([-1 if axis == axis_at else 1 for axis in range(entries.ndim)]) for axis_at in (source, target)]
    chosen = jax.random.permutation(own_key, parts)[partner]
    strong = (owner == chosen) | (owner == (partner + parts // 2) % parts)
    return jnp.where(strong, factor * entries, entries)


def level_of(rng, shape, pieces, least, top_value):
    loudness, own = 1.0, jax.random.fold_in(rng, 6)
    for position, parts in pieces:
        heights = jnp.exp(jax.random.uniform(jax.random.fold_in(own, position), (parts,), jnp.float32, least / len(pieces), top_value / len(pieces)))
        loudness = loudness * jnp.repeat(heights, shape[position] // parts).reshape([-1 if axis == position else 1 for axis in range(len(shape))])
    return loudness


def noise(key, dims, deviation, most, pieces=(), kind=jnp.bfloat16):
    values = jax.random.normal(key, dims, jnp.float32) * deviation
    if len(pieces) > 0:
        values = level_of(key, dims, pieces, -0.22, 0.18) * values
    return jnp.clip(values, min=-most, max=most).astype(kind)


def heavy_noise(own_key, shape, deviation, reach, cuts, heavy, held_as=jnp.bfloat16):
    array = deviation * jax.random.normal(own_key, shape, jnp.float32)
    if cuts:
        array = array * level_of(own_key, shape, cuts, -0.22, 0.18)
    return jnp.clip(spiked(array, jax.random.fold_in(own_key, 3), *heavy), -reach, reach).astype(held_as)


def setup_inputs(seed: int = 0) -> dict:
    splits = jax.random.split(jax.random.key(seed), 6)
    acts = heavy_noise(splits[0], (N_GRP, ROWS, BLK), 1.0, 16.0, ((0, 8), (1, 64)), (1, 2, 64, 4.0))
    grads = heavy_noise(splits[1], (N_GRP, ROWS, BLK), 1.0, 16.0, ((0, 8), (1, 64)), (1, 2, 64, 4.0))
    tile_expert = plant(jax.random.randint(splits[2], (N_GRP, TILES_ALL), 0, EXP_GRP), jax.random.fold_in(splits[2], 1), 0, EXP_GRP - 1).astype(jnp.int32)
    tile_rows = plant(jax.random.randint(splits[3], (N_GRP, TILES_ALL), 1, TROWS + 1), jax.random.fold_in(splits[3], 1), 1, TROWS).astype(jnp.int32)
    previous = noise(splits[4], (BLK, EXPERTS, 2, BLK), 0.03, 0.18, ((0, 64), (3, 8)), jnp.float32)
    return {"acts": acts, "grads": grads, "tile_expert": tile_expert, "tile_rows": tile_rows, "previous": previous}


def group_sums(operands):
    acts_group, grads_group, expert_group, rows_group = operands
    tile_acts = acts_group.reshape(TILES_ALL, TROWS, BLK).astype(jnp.float32)
    tile_grads = grads_group.reshape(TILES_ALL, TROWS, BLK).astype(jnp.float32)
    positions = jnp.arange(TROWS)
    expert_ids = jnp.arange(EXP_GRP)

    def tile_step(running, item):
        acts_tile, grads_tile, expert_id, live_count = item
        live_rows = (positions < live_count).astype(jnp.float32)[:, None]
        left = jnp.dot((acts_tile * live_rows).T, acts_tile, precision=lax.Precision.HIGHEST)
        right = jnp.dot((grads_tile * live_rows).T, grads_tile, precision=lax.Precision.HIGHEST)
        expert_pick = (expert_ids == expert_id).astype(jnp.float32)
        return running + expert_pick[:, None, None, None] * jnp.stack([left, right])[None], None

    initial = jnp.zeros((EXP_GRP, 2, BLK, BLK), jnp.float32)
    totals, unused = lax.scan(tile_step, initial, (tile_acts, tile_grads, expert_group, rows_group))
    return totals


def reference(acts, grads, tile_expert, tile_rows, previous):
    totals = lax.map(group_sums, (acts, grads, tile_expert, tile_rows))
    totals = totals.reshape(EXPERTS, 2, BLK, BLK).transpose(2, 0, 1, 3)
    return previous + totals * (1.0 / ROWS)
```

```python
import functools

import jax
import jax.numpy as jnp
from jax import lax
from jax.experimental import pallas as pl
from jax.experimental.pallas import tpu as pltpu
from jax.sharding import PartitionSpec as P

MESH = pl.DeviceIdType.MESH
F32 = jnp.float32
SUB = 8


def kernel(
    n,
    scale,
    acts_hbm,
    grads_hbm,
    tile_expert,
    tile_rows,
    previous_hbm,
    out_ref,
    acts_ref,
    grads_ref,
    previous_ref,
    full,
    sums,
    landed,
    crossed,
    pieces,
    corner,
    final,
    spread,
    in_sem,
    ring_send,
    ring_recv,
    cross_send,
    cross_recv,
    last_send,
    last_recv,
):
    half = n // 2
    blk = SUB * n
    rows = acts_ref.shape[0]
    tile_count = tile_rows.shape[1]
    tile_len = rows // tile_count
    chunk_rows = SUB * (n + 1) * half
    part_rows = chunk_rows // 2
    region = SUB * (half + 1)
    tok = lax.axis_index("tok")
    grp = lax.axis_index("grp")
    y, z = tok // n, tok % n

    def device(yy, zz, gg):
        return {"tok": yy * n + zz, "grp": gg}

    loads = [
        pltpu.make_async_copy(acts_hbm.at[0], acts_ref, in_sem.at[0]),
        pltpu.make_async_copy(grads_hbm.at[0], grads_ref, in_sem.at[1]),
        pltpu.make_async_copy(previous_hbm, previous_ref, in_sem.at[2]),
    ]
    for load in loads:
        load.start()

    barrier = pltpu.get_barrier_semaphore()
    for step in range(1, n):
        for peer in (
            device((y + step) % n, z, grp),
            device(y, (z + step) % n, grp),
            device(y, z, (grp + step) % n),
        ):
            pl.semaphore_signal(barrier, inc=1, device_id=peer, device_id_type=MESH)

    lane = lax.broadcasted_iota(jnp.int32, (1, rows), 1)
    inside = lane % tile_len
    picks = []
    for expert in range(2):
        limit = jnp.zeros((1, rows), jnp.int32)
        for tile in range(tile_count):
            count = jnp.where(tile_expert[0, tile] == expert, tile_rows[0, tile], 0)
            limit = jnp.where(lane // tile_len == tile, count, limit)
        picks.append(jnp.where(inside < limit, 1.0, 0.0).astype(jnp.bfloat16))
    for side, ref in ((0, acts_ref), (1, grads_ref)):
        loads[side].wait()
        values = ref[...]
        flipped = values.T
        for expert in range(2):
            full[expert, side] = jnp.dot(
                flipped * picks[expert], values, preferred_element_type=F32
            )

    low = lax.broadcasted_iota(jnp.int32, (blk, 2 * blk), 1) < blk
    for i in range(n):
        for d in range(half + 1):
            j = (i + d) % n
            for expert in range(2):
                if d == half and expert != (0 if i < half else 1):
                    continue
                at = (pl.ds(i * blk, blk), pl.ds((j // 2) * 2 * blk, 2 * blk))
                left, right = full[expert, 0, at[0], at[1]], full[expert, 1, at[0], at[1]]
                if j % 2 == 0:
                    right = pltpu.roll(right, blk, 1)
                else:
                    left = pltpu.roll(left, blk, 1)
                pair = jnp.where(low, left, right)
                if d == 0 and expert == 0:
                    for oz in range(n):
                        tile = pair[oz * SUB : (oz + 1) * SUB]
                        if (i + oz) % 2 == 0:
                            first = (oz // 2) * (n + 1) * SUB
                            first += (oz % 2) * SUB * (half + (i + 1) % 2) + SUB * half
                            sums[0, i, first : first + SUB] = tile
                        else:
                            first = (i // 2) * (n + 1) * SUB
                            first += (i % 2) * SUB * (half + oz % 2) + SUB * half
                            sums[1, oz, first : first + SUB] = tile
                    continue
                if d == 0:
                    oz = 0
                elif d == half:
                    oz = n - 1
                else:
                    oz = 2 * d - 1 + expert
                oy = (i + d // 2) % n
                first = (oz // 2) * (n + 1) * SUB + (oz % 2) * SUB * (half + (oy + 1) % 2)
                sums[0, oy, first : first + blk // 2] = pair[: blk // 2]
                first = (oy // 2) * (n + 1) * SUB + (oy % 2) * SUB * (half + oz % 2)
                sums[1, oz, first : first + blk // 2] = pair[blk // 2 :]
    for chunk in range(n):
        for dim in range(2):
            sums[dim, chunk, chunk_rows : chunk_rows + SUB] = jnp.zeros((SUB, 2 * blk), F32)

    pl.semaphore_wait(barrier, 3 * (n - 1))

    streams = []
    for dim in range(2):
        here = y if dim == 0 else z
        for sign in (-1, 1):
            there = (here + sign + n) % n
            peer = device(there, z, grp) if dim == 0 else device(y, there, grp)
            streams.append((dim, sign, here, peer))

    def ring_place(stream, m):
        dim, sign, here, peer = streams[stream]
        away = half - m // 2 if m % 2 == 0 else half - 1 - (m - 1) // 2
        part = m % 2 if sign < 0 else (m + 1) % 2
        return dim, (here + sign * away + n) % n, pl.ds(part * part_rows, part_rows)

    def ring_copy(stream, m):
        return pltpu.make_async_remote_copy(
            src_ref=sums.at[ring_place(stream, m)],
            dst_ref=landed.at[stream, m],
            send_sem=ring_send.at[stream, m],
            recv_sem=ring_recv.at[stream, m],
            device_id=streams[stream][3],
            device_id_type=MESH,
        )

    for m in range(n - 1):
        for stream in range(4):
            if m >= 2:
                at = ring_place(stream, m)
                ring_copy(stream, m - 2).wait_recv()
                sums[at] = sums[at] + landed[stream, m - 2]
            ring_copy(stream, m).start()
    for m in (n - 3, n - 2):
        for stream in range(4):
            ring_copy(stream, m).wait_recv()
    for dim in range(2):
        here = y if dim == 0 else z
        for part in range(2):
            at = pl.ds(part * part_rows, part_rows)
            downs, ups = (n - 2, n - 3) if part == 0 else (n - 3, n - 2)
            sums[dim, here, at] = (
                sums[dim, here, at] + landed[2 * dim, downs] + landed[2 * dim + 1, ups]
            )

    def first_row(dim, other):
        extra = (y + 1) % 2 if dim == 0 else z % 2
        return pl.multiple_of(
            (other // 2) * ((n + 1) * SUB) + (other % 2) * (SUB * (half + extra)), SUB
        )

    def cross_copy(dim, step):
        if dim == 0:
            chunk, other = y, (z + step) % n
            peer = device(y, other, grp)
        else:
            chunk, other = z, (y + step) % n
            peer = device(other, z, grp)
        return pltpu.make_async_remote_copy(
            src_ref=sums.at[dim, chunk, pl.ds(first_row(dim, other), region)],
            dst_ref=crossed.at[dim, step],
            send_sem=cross_send.at[dim, step],
            recv_sem=cross_recv.at[dim, step],
            device_id=peer,
            device_id_type=MESH,
        )

    order = sorted(range(1, n), key=lambda step: (-min(step, n - step), step))
    for step in order:
        for dim in range(2):
            cross_copy(dim, step).start()
    owned = []
    for dim in range(2):
        chunk, other = (y, z) if dim == 0 else (z, y)
        total = sums[dim, chunk, pl.ds(first_row(dim, other), region)]
        for step in reversed(order):
            cross_copy(dim, step).wait_recv()
            total = total + crossed[dim, step]
        owned.append(total)

    d = (z + 1) // 2
    i = (y - d // 2 + n) % n
    j = (i + d) % n
    expert = jnp.where(
        z == n - 1, jnp.where(i < half, 0, 1), jnp.where(z == 0, 1, (z + 1) % 2)
    )
    block = jnp.concatenate([owned[0][: blk // 2], owned[1][: blk // 2]], axis=0)
    mirror = jnp.concatenate([block, pltpu.roll(block, blk, 1)], axis=0).T[:blk]
    for tile in range(n):
        pieces[0, tile] = block[tile * SUB : (tile + 1) * SUB]
        pieces[1, tile] = mirror[tile * SUB : (tile + 1) * SUB]
    corner[...] = jnp.where(
        (y + z) % 2 == 0, owned[0][blk // 2 : region], owned[1][blk // 2 : region]
    )
    slot = grp * 2 + expert

    def last_copies():
        for step in [0] + order[::-1]:
            zz = (z + step) % n
            yield step, None, pieces.at[0, zz], slot, (i, zz, j)
            yield n + step, z > 0, pieces.at[1, zz], slot, (j, zz, i)
        yield 2 * n, None, corner, grp * 2, (y, z, y)

    def last_copy(index, src, which, to):
        return pltpu.make_async_remote_copy(
            src_ref=src,
            dst_ref=final.at[pl.ds(pl.multiple_of(which * SUB, SUB), SUB)],
            send_sem=last_send.at[index],
            recv_sem=last_recv,
            device_id=device(*to),
            device_id_type=MESH,
        )

    def leaves(used, to):
        stays = (to[0] == y) & (to[1] == z) & (to[2] == grp)
        leave = jnp.logical_not(stays)
        return (leave, stays) if used is None else (used & leave, used & stays)

    for index, used, src, which, to in reversed(list(last_copies())):
        leave, stays = leaves(used, to)

        @pl.when(leave)
        def _():
            last_copy(index, src, which, to).start()

        @pl.when(stays)
        def _():
            pltpu.make_async_copy(
                src, final.at[pl.ds(pl.multiple_of(which * SUB, SUB), SUB)], last_recv
            ).start()

    loads[2].wait()
    pltpu.make_async_copy(final, final, last_recv).wait()
    experts = 2 * n
    for row in range(SUB):
        pair = final[pl.ds(row, experts, stride=SUB), :] * scale
        other = pltpu.roll(pair, blk, 1)
        spread[pl.ds(row * 2 * experts, experts, stride=2), :] = pair
        spread[pl.ds(row * 2 * experts + 1, experts, stride=2), :] = other
    out_ref[...] = previous_ref[...] + spread[:, :blk]

    for m in range(n - 1):
        for stream in range(4):
            ring_copy(stream, m).wait_send()
    for step in order:
        for dim in range(2):
            cross_copy(dim, step).wait_send()
    for index, used, src, which, to in last_copies():

        @pl.when(leaves(used, to)[0])
        def _():
            last_copy(index, src, which, to).wait_send()


def solution(mesh):
    n = mesh.shape["grp"]
    tok_count = mesh.shape["tok"]

    def body(acts, grads, tile_expert, tile_rows, previous):
        rows, blk_all = acts.shape[1:]
        own_rows, experts, sides, cols = previous.shape
        half = n // 2
        wide = 2 * cols
        chunk_rows = SUB * (n + 1) * half
        region = SUB * (half + 1)
        flat = own_rows * experts * sides
        scale = 1.0 / (rows * tok_count)
        result = pl.pallas_call(
            functools.partial(kernel, n, scale),
            out_shape=jax.ShapeDtypeStruct((flat, cols), F32),
            in_specs=[
                pl.BlockSpec(memory_space=pl.ANY),
                pl.BlockSpec(memory_space=pl.ANY),
                pl.BlockSpec(memory_space=pltpu.SMEM),
                pl.BlockSpec(memory_space=pltpu.SMEM),
                pl.BlockSpec(memory_space=pl.ANY),
            ],
            out_specs=pl.BlockSpec(memory_space=pltpu.VMEM),
            scratch_shapes=[
                pltpu.VMEM((rows, blk_all), jnp.bfloat16),
                pltpu.VMEM((rows, blk_all), jnp.bfloat16),
                pltpu.VMEM((flat, cols), F32),
                pltpu.VMEM((2, 2, blk_all, blk_all), F32),
                pltpu.VMEM((2, n, chunk_rows + SUB, wide), F32),
                pltpu.VMEM((4, n - 1, chunk_rows // 2, wide), F32),
                pltpu.VMEM((2, n, region, wide), F32),
                pltpu.VMEM((2, n, SUB, wide), F32),
                pltpu.VMEM((SUB, wide), F32),
                pltpu.VMEM((experts * SUB, wide), F32),
                pltpu.VMEM((flat, wide), F32),
                pltpu.SemaphoreType.DMA((3,)),
                pltpu.SemaphoreType.DMA((4, n - 1)),
                pltpu.SemaphoreType.DMA((4, n - 1)),
                pltpu.SemaphoreType.DMA((2, n)),
                pltpu.SemaphoreType.DMA((2, n)),
                pltpu.SemaphoreType.DMA((2 * n + 1,)),
                pltpu.SemaphoreType.DMA,
            ],
            compiler_params=pltpu.CompilerParams(
                collective_id=0, has_side_effects=True, vmem_limit_bytes=62 * 1024 * 1024
            ),
        )(acts, grads, tile_expert, tile_rows, previous.reshape(flat, cols))
        return result.reshape(previous.shape)

    return jax.shard_map(
        body,
        mesh=mesh,
        in_specs=(
            P("grp", "tok", None),
            P("grp", "tok", None),
            P("grp", "tok"),
            P("grp", "tok"),
            P("tok", None, None, "grp"),
        ),
        out_specs=P("tok", None, None, "grp"),
        check_vma=False,
    )
```

```python
import functools

import jax
import jax.numpy as jnp
from jax import lax
from jax.experimental import pallas as pl
from jax.experimental.pallas import tpu as pltpu
from jax.sharding import PartitionSpec as P

MESH = pl.DeviceIdType.MESH
F32 = jnp.float32
SUB = 8


def kernel(
    n,
    scale,
    acts_hbm,
    grads_hbm,
    expert_hbm,
    rows_hbm,
    out_ref,
    acts_ref,
    grads_ref,
    tile_expert,
    tile_rows,
    full,
    sums,
    landed,
    crossed,
    pieces,
    corner,
    final,
    spread,
    in_sem,
    ring_send,
    ring_recv,
    cross_send,
    cross_recv,
    last_send,
    last_recv,
):
    half = n // 2
    blk = SUB * n
    rows = acts_ref.shape[0]
    tile_count = tile_rows.shape[1]
    tile_len = rows // tile_count
    pieces_all = n // 2
    piece_rows = SUB * (n + 1)
    region = SUB * (half + 1)
    tok = lax.axis_index("tok")
    grp = lax.axis_index("grp")
    y, z = tok // n, tok % n

    def region_first(dim, chunk, other):
        longer = (chunk + other + 1 + dim) % 2
        return (other // 2) * ((n + 1) * SUB) + longer * (SUB * half)

    def device(yy, zz, gg):
        return {"tok": yy * n + zz, "grp": gg}

    loads = [
        pltpu.make_async_copy(acts_hbm.at[0], acts_ref, in_sem.at[0]),
        pltpu.make_async_copy(grads_hbm.at[0], grads_ref, in_sem.at[1]),
        pltpu.make_async_copy(expert_hbm, tile_expert, in_sem.at[2]),
        pltpu.make_async_copy(rows_hbm, tile_rows, in_sem.at[3]),
    ]
    for load in loads:
        load.start()

    barrier = pltpu.get_barrier_semaphore()
    near = [device((y + step) % n, z, grp) for step in (1, n - 1)]
    near += [device(y, (z + step) % n, grp) for step in (1, n - 1)]
    near += [device(y, z, (grp + step) % n) for step in range(1, n)]
    for peer in near:
        pl.semaphore_signal(barrier, inc=1, device_id=peer, device_id_type=MESH)

    loads[2].wait()
    loads[3].wait()
    lane = lax.broadcasted_iota(jnp.int32, (1, rows), 1)
    inside = lane % tile_len
    picks = []
    for expert in range(2):
        limit = jnp.zeros((1, rows), jnp.int32)
        for tile in range(tile_count):
            count = jnp.where(tile_expert[0, tile] == expert, tile_rows[0, tile], 0)
            limit = jnp.where(lane // tile_len == tile, count, limit)
        picks.append(jnp.where(inside < limit, 1.0, 0.0).astype(jnp.bfloat16))
    for side, ref in ((0, acts_ref), (1, grads_ref)):
        loads[side].wait()
        values = ref[...]
        flipped = values.T
        for expert in range(2):
            full[expert, side] = jnp.dot(
                flipped * picks[expert], values, preferred_element_type=F32
            )

    low = lax.broadcasted_iota(jnp.int32, (blk, 2 * blk), 1) < blk
    for i in range(n):
        for d in range(half + 1):
            j = (i + d) % n
            for expert in range(2):
                if d == half and expert != (0 if i < half else 1):
                    continue
                at = (pl.ds(i * blk, blk), pl.ds((j // 2) * 2 * blk, 2 * blk))
                left, right = full[expert, 0, at[0], at[1]], full[expert, 1, at[0], at[1]]
                if j % 2 == 0:
                    right = pltpu.roll(right, blk, 1)
                else:
                    left = pltpu.roll(left, blk, 1)
                pair = jnp.where(low, left, right)
                if d == 0 and expert == 0:
                    for oz in range(n):
                        tile = pair[oz * SUB : (oz + 1) * SUB]
                        dim = (i + oz) % 2
                        chunk, other = (i, oz) if dim == 0 else (oz, i)
                        first = region_first(dim, chunk, other) + SUB * half
                        sums[dim, chunk, first : first + SUB] = tile
                    continue
                if d == 0:
                    oz = 0
                elif d == half:
                    oz = n - 1
                else:
                    oz = 2 * d - 1 + expert
                oy = (i + d // 2) % n
                first = region_first(0, oy, oz)
                sums[0, oy, first : first + blk // 2] = pair[: blk // 2]
                first = region_first(1, oz, oy)
                sums[1, oz, first : first + blk // 2] = pair[blk // 2 :]

    pl.semaphore_wait(barrier, len(near))

    streams = []
    for dim in range(2):
        here = y if dim == 0 else z
        for sign in (-1, 1):
            there = (here + sign + n) % n
            peer = device(there, z, grp) if dim == 0 else device(y, there, grp)
            streams.append((dim, sign, here, peer))

    rank = sorted(range(pieces_all), key=lambda r: (-min(r, pieces_all - r), r))

    def messages(sign):
        far = [r for r in range(pieces_all) if (r % 2 == 0) == (sign < 0)]
        close = [r for r in range(pieces_all) if r not in far]
        plan = [(r, half) for r in far]
        for away in range(half - 1, 1, -1):
            plan += [(r, away) for r in close] + [(r, away) for r in far]
        for pair in zip(close, far):
            plan += [(r, 1) for r in pair]
        return plan

    plans = [messages(sign) for _, sign, _, _ in streams]
    total_messages = len(plans[0])

    def piece_first(dim, r):
        along = z if dim == 0 else y
        return pl.multiple_of((along // 2 + rank[r]) % pieces_all * piece_rows, SUB)

    def ring_place(stream, m):
        dim, sign, here, peer = streams[stream]
        r, away = plans[stream][m]
        return dim, (here + sign * away + n) % n, pl.ds(piece_first(dim, r), piece_rows)

    def ring_copy(stream, m):
        return pltpu.make_async_remote_copy(
            src_ref=sums.at[ring_place(stream, m)],
            dst_ref=landed.at[stream, m],
            send_sem=ring_send.at[stream, m],
            recv_sem=ring_recv.at[stream, m],
            device_id=streams[stream][3],
            device_id_type=MESH,
        )

    for m in range(total_messages):
        for stream in range(4):
            r, away = plans[stream][m]
            if (r, away + 1) in plans[stream]:
                before = plans[stream].index((r, away + 1))
                at = ring_place(stream, m)
                ring_copy(stream, before).wait_recv()
                sums[at] = sums[at] + landed[stream, before]
            ring_copy(stream, m).start()

    def first_row(dim, other):
        return pl.multiple_of(region_first(dim, y if dim == 0 else z, other), SUB)

    def cross_copy(dim, r, which):
        mine = z if dim == 0 else y
        if rank[r] == 0:
            other = mine + 1 - 2 * (mine % 2)
        else:
            other = (mine // 2 + rank[r]) % pieces_all * 2 + which
        peer = device(y, other, grp) if dim == 0 else device(other, z, grp)
        return pltpu.make_async_remote_copy(
            src_ref=sums.at[dim, y if dim == 0 else z, pl.ds(first_row(dim, other), region)],
            dst_ref=crossed.at[dim, (other - mine + n) % n],
            send_sem=cross_send.at[dim, 2 * r + which],
            recv_sem=cross_recv.at[dim],
            device_id=peer,
            device_id_type=MESH,
        )

    def cross_copies():
        for r in range(pieces_all):
            for dim in range(2):
                for which in range(1 if rank[r] == 0 else 2):
                    yield dim, r, which

    for r in range(pieces_all):
        for dim in range(2):
            here = y if dim == 0 else z
            at = (dim, here, pl.ds(piece_first(dim, r), piece_rows))
            total = sums[at]
            for stream in (2 * dim, 2 * dim + 1):
                m = plans[stream].index((r, 1))
                ring_copy(stream, m).wait_recv()
                total = total + landed[stream, m]
            sums[at] = total
        for dim in range(2):
            for which in range(1 if rank[r] == 0 else 2):
                cross_copy(dim, r, which).start()
    owned = []
    for dim in range(2):
        chunk, other = (y, z) if dim == 0 else (z, y)
        total = sums[dim, chunk, pl.ds(first_row(dim, other), region)]
        arrived = crossed.at[dim, pl.ds(1, n - 1)]
        pltpu.make_async_copy(arrived, arrived, cross_recv.at[dim]).wait()
        for step in range(1, n):
            total = total + crossed[dim, step]
        owned.append(total)

    d = (z + 1) // 2
    i = (y - d // 2 + n) % n
    j = (i + d) % n
    expert = jnp.where(
        z == n - 1, jnp.where(i < half, 0, 1), jnp.where(z == 0, 1, (z + 1) % 2)
    )
    block = jnp.concatenate([owned[0][: blk // 2], owned[1][: blk // 2]], axis=0)
    mirror = jnp.concatenate([block, pltpu.roll(block, blk, 1)], axis=0).T[:blk]
    for tile in range(n):
        pieces[0, tile] = block[tile * SUB : (tile + 1) * SUB]
        pieces[1, tile] = mirror[tile * SUB : (tile + 1) * SUB]
    corner[...] = jnp.where(
        (y + z) % 2 == 0, owned[0][blk // 2 : region], owned[1][blk // 2 : region]
    )
    slot = grp * 2 + expert

    order = sorted(range(1, n), key=lambda step: (-min(step, n - step), step))

    def last_copies():
        for step in [0] + order[::-1]:
            zz = (z + step) % n
            yield step, None, pieces.at[0, zz], slot, (i, zz, j)
            yield n + step, z > 0, pieces.at[1, zz], slot, (j, zz, i)
        yield 2 * n, None, corner, grp * 2, (y, z, y)

    def last_copy(index, src, which, to):
        return pltpu.make_async_remote_copy(
            src_ref=src,
            dst_ref=final.at[pl.ds(pl.multiple_of(which * SUB, SUB), SUB)],
            send_sem=last_send.at[index],
            recv_sem=last_recv,
            device_id=device(*to),
            device_id_type=MESH,
        )

    def leaves(used, to):
        stays = (to[0] == y) & (to[1] == z) & (to[2] == grp)
        leave = jnp.logical_not(stays)
        return (leave, stays) if used is None else (used & leave, used & stays)

    for index, used, src, which, to in reversed(list(last_copies())):
        leave, stays = leaves(used, to)

        @pl.when(leave)
        def _():
            last_copy(index, src, which, to).start()

        @pl.when(stays)
        def _():
            pltpu.make_async_copy(
                src, final.at[pl.ds(pl.multiple_of(which * SUB, SUB), SUB)], last_recv
            ).start()

    pltpu.make_async_copy(final, final, last_recv).wait()
    experts = 2 * n
    for row in range(SUB):
        pair = final[pl.ds(row, experts, stride=SUB), :] * scale
        other = pltpu.roll(pair, blk, 1)
        spread[pl.ds(row * 2 * experts, experts, stride=2), :] = pair
        spread[pl.ds(row * 2 * experts + 1, experts, stride=2), :] = other
    out_ref[...] = spread[:, :blk]

    for m in range(total_messages):
        for stream in range(4):
            ring_copy(stream, m).wait_send()
    for dim, r, which in cross_copies():
        cross_copy(dim, r, which).wait_send()
    for index, used, src, which, to in last_copies():

        @pl.when(leaves(used, to)[0])
        def _():
            last_copy(index, src, which, to).wait_send()


def solution(mesh):
    n = mesh.shape["grp"]
    tok_count = mesh.shape["tok"]

    def body(acts, grads, tile_expert, tile_rows, previous):
        rows, blk_all = acts.shape[1:]
        own_rows, experts, sides, cols = previous.shape
        half = n // 2
        wide = 2 * cols
        chunk_rows = SUB * (n + 1) * half
        region = SUB * (half + 1)
        messages = (n - 1) * half // 2
        flat = own_rows * experts * sides
        scale = 1.0 / (rows * tok_count)
        operands = (acts, grads, tile_expert, tile_rows)
        result = pl.pallas_call(
            functools.partial(kernel, n, scale),
            out_shape=jax.ShapeDtypeStruct((flat, cols), F32),
            in_specs=[
                pl.BlockSpec(memory_space=pltpu.HBM),
                pl.BlockSpec(memory_space=pltpu.HBM),
                pl.BlockSpec(memory_space=pltpu.HBM),
                pl.BlockSpec(memory_space=pltpu.HBM),
            ],
            out_specs=pl.BlockSpec(memory_space=pltpu.VMEM),
            scratch_shapes=[
                pltpu.VMEM((rows, blk_all), jnp.bfloat16),
                pltpu.VMEM((rows, blk_all), jnp.bfloat16),
                pltpu.SMEM(tile_expert.shape, jnp.int32),
                pltpu.SMEM(tile_rows.shape, jnp.int32),
                pltpu.VMEM((2, 2, blk_all, blk_all), F32),
                pltpu.VMEM((2, n, chunk_rows, wide), F32),
                pltpu.VMEM((4, messages, SUB * (n + 1), wide), F32),
                pltpu.VMEM((2, n, region, wide), F32),
                pltpu.VMEM((2, n, SUB, wide), F32),
                pltpu.VMEM((SUB, wide), F32),
                pltpu.VMEM((experts * SUB, wide), F32),
                pltpu.VMEM((flat, wide), F32),
                pltpu.SemaphoreType.DMA((4,)),
                pltpu.SemaphoreType.DMA((4, messages)),
                pltpu.SemaphoreType.DMA((4, messages)),
                pltpu.SemaphoreType.DMA((2, n)),
                pltpu.SemaphoreType.DMA((2,)),
                pltpu.SemaphoreType.DMA((2 * n + 1,)),
                pltpu.SemaphoreType.DMA,
            ],
            compiler_params=pltpu.CompilerParams(
                collective_id=0, has_side_effects=True, vmem_limit_bytes=32 * 1024 * 1024
            ),
        )(*(pltpu.with_memory_space_constraint(x, pltpu.HBM) for x in operands))
        return previous + result.reshape(previous.shape)

    return jax.shard_map(
        body,
        mesh=mesh,
        in_specs=(
            P("grp", "tok", None),
            P("grp", "tok", None),
            P("grp", "tok"),
            P("grp", "tok"),
            P("tok", None, None, "grp"),
        ),
        out_specs=P("tok", None, None, "grp"),
        check_vma=False,
    )
```
